256 devices in a mesh: tm: 64 (over y, x, z_lo), chan: 4 (over z_hi, core).
Axes of the slice: x: 4, y: 4, z: 8 (z_hi: 2, z_lo: 4; z = z_hi * 4 + z_lo), core: 2. Of those that a mesh axis runs over, the one named last changes fastest.
Arguments:
- inputs: bfloat16 [32768, 8192], P('tm', 'chan'), may hold values from -52 to 52
- gate_logits: bfloat16 [32768, 8192], P(('tm', 'chan')), may hold values from -5 to 5
- step_sizes: bfloat16 [32768, 64], P('tm', 'chan'), may hold values from 0.3 to 229376, as said below
- decay_rates: float32 [8192], replicated, as said below
- skip_gain: float32 [8192], replicated, may hold values from 0.3 to 0.8
- norm_gain: float32 [8192], replicated, may hold values from 0.25 to 1.75
Outputs:
- outputs: bfloat16 [32768, 8192], P(('tm', 'chan'))
The draws below stay inside these ranges and needn't reach their ends.
Inputs may be any that keep to these rules, and one draw needn't show every extreme that they name: `step_sizes`: every step size is positive. `decay_rates`: every rate is positive.
All inputs are finite; a program needn't handle non-finite values.
Results may differ from the reference program's by a relative error of at most 0.0049.
Values may be sent and summed in bfloat16 or wider, within the bound.
A program may use at most 64 MiB of HBM per device.

```python
import math
import jax
import jax.numpy as jnp
from jax import lax

N = 8192
HEAD_SIZE = 128
HEADS = 64
TOK_DEV = 512
TOKENS = 32768


def head_profile(key):
    anchor = jax.random.fold_in(key, 7103)
    ranking = jax.random.permutation(jax.random.fold_in(anchor, 1), HEADS)
    fast_count = HEADS // 2
    is_fast = ranking < fast_count
    fast_low = math.log(0.75 / TOK_DEV)
    fast_high = math.log(1.0 / 25.0)
    jitter = jax.random.uniform(jax.random.fold_in(anchor, 2), (HEADS,), jnp.float32, 0.0, 1.0)
    place = (ranking.astype(jnp.float32) + jitter) / float(fast_count)
    place = jnp.clip(place, 0.0, 1.0)
    fast_rate = jnp.exp(fast_low + place * (fast_high - fast_low))
    slow_rate = jnp.exp(jax.random.uniform(jax.random.fold_in(anchor, 3), (HEADS,), jnp.float32, math.log(1.3), math.log(1.8))) / TOKENS
    return jnp.where(is_fast, fast_rate, slow_rate)


def draw_decay_rates(key, part):
    head_rate = head_profile(key)
    factor = jnp.exp(jax.random.uniform(jax.random.fold_in(key, 11), (N,), jnp.float32, math.log(0.7), math.log(1.45)))
    return (jnp.repeat(head_rate, HEAD_SIZE) * factor).astype(jnp.float32)


def draw_step_sizes(key, part):
    head_rate = head_profile(key)
    anchor = jax.random.fold_in(key, 29)
    block_count = TOKENS // TOK_DEV
    device_factor = jnp.exp(jax.random.uniform(jax.random.fold_in(anchor, 1), (block_count,), jnp.float32, math.log(0.6), math.log(1.6)))
    token_factor = jnp.exp(jax.random.uniform(jax.random.fold_in(anchor, 2), (TOKENS, HEADS), jnp.float32, math.log(0.7), math.log(1.4)))
    sizes_now = jnp.repeat(device_factor, TOK_DEV)[:, None] * token_factor
    places = jax.random.randint(jax.random.fold_in(anchor, 3), (2, HEADS), 0, TOKENS)
    strength = jnp.exp(jax.random.uniform(jax.random.fold_in(anchor, 4), (2, HEADS), jnp.float32, math.log(0.22), math.log(0.5)))
    positions = jnp.arange(TOKENS, dtype=jnp.int32)[:, None]
    first_hit = positions == places[0][None, :]
    sizes_now = jnp.where(first_hit, (strength[0] / head_rate)[None, :], sizes_now)
    second_hit = positions == places[1][None, :]
    sizes_now = jnp.where(second_hit, (strength[1] / head_rate)[None, :], sizes_now)
    return sizes_now.astype(jnp.bfloat16)


def draw_inputs(key, part):
    anchor = jax.random.fold_in(key, 53)
    noise = jnp.clip(jax.random.normal(jax.random.fold_in(anchor, 1), (TOKENS, N), jnp.float32), -4.0, 4.0)
    row_scale = jnp.exp(jax.random.uniform(jax.random.fold_in(anchor, 2), (TOKENS, 1), jnp.float32, -0.5 * math.log(10.0), 0.5 * math.log(10.0)))
    column_scale = jnp.exp(jax.random.uniform(jax.random.fold_in(anchor, 3), (1, N), jnp.float32, -0.5 * math.log(10.0), 0.5 * math.log(10.0)))
    values = noise * row_scale * column_scale
    return values.astype(jnp.bfloat16)


def shard_levels(rng, extent, pieces, least, largest):
    loudness, own = 1.0, jax.random.fold_in(rng, 6)
    for axis_at, shards_of in pieces:
        heights = jnp.exp(jax.random.uniform(jax.random.fold_in(own, axis_at), (shards_of,), jnp.float32, least / len(pieces), largest / len(pieces)))
        loudness = loudness * jnp.repeat(heights, extent[axis_at] // shards_of).reshape([-1 if axis == axis_at else 1 for axis in range(len(extent))])
    return loudness


def normal_values(key, extent, scale, bound, pieces=(), held_as=jnp.bfloat16):
    values = scale * jax.random.normal(key, extent, jnp.float32)
    if pieces:
        values = values * shard_levels(key, extent, pieces, -0.22, 0.18)
    return jnp.clip(values, -bound, bound).astype(held_as)


def setup_inputs(seed: int = 0) -> dict:
    seeds = jax.random.split(jax.random.key(seed), 7)
    inputs = draw_inputs(jax.random.fold_in(seeds[6], 71), 0)
    gate_logits = normal_values(seeds[1], (TOKENS, N), 1.0, 5.0, ((0, 256),))
    step_sizes = draw_step_sizes(jax.random.fold_in(seeds[6], 71), 0)
    decay_rates = draw_decay_rates(jax.random.fold_in(seeds[6], 71), 0)
    skip_gain = jnp.clip(jax.random.uniform(seeds[4], (N,), jnp.float32, 0.3, 0.8), 0.3, 0.8)
    norm_gain = jnp.clip(1.0 + 0.15 * jax.random.normal(seeds[5], (N,), jnp.float32), 0.25, 1.75)
    return {"inputs": inputs, "gate_logits": gate_logits, "step_sizes": step_sizes, "decay_rates": decay_rates, "skip_gain": skip_gain, "norm_gain": norm_gain}


norm_epsilon = 1e-05

def combine_pairs(earlier, later):
    return (earlier[0] * later[0], later[0] * earlier[1] + later[1])

def reference(inputs, gate_logits, step_sizes, decay_rates, skip_gain, norm_gain):
    block_count = TOKENS // TOK_DEV
    input_blocks = inputs.reshape(block_count, TOK_DEV, N)
    gate_blocks = gate_logits.reshape(block_count, TOK_DEV, N)
    step_blocks = step_sizes.reshape(block_count, TOK_DEV, HEADS)

    def advance(carried, block):
        block_inputs, block_gate, block_steps = block
        widened = jnp.repeat(block_steps.astype(jnp.float32), HEAD_SIZE, axis=1) * decay_rates[None, :]
        decays = jnp.exp(-widened)
        values = block_inputs.astype(jnp.float32)
        drives = jnp.sqrt(-jnp.expm1(-2.0 * widened)) * values
        products, local_states = lax.associative_scan(combine_pairs, (decays, drives), axis=0)
        states = local_states + products * carried[None, :]
        mixed = (states + skip_gain[None, :] * values).astype(jnp.bfloat16)
        mixed = lax.optimization_barrier(mixed)
        gated = mixed.astype(jnp.float32) * jax.nn.silu(block_gate.astype(jnp.float32))
        factor = lax.rsqrt(lax.optimization_barrier(jnp.mean(gated * gated, axis=1, keepdims=True)) + norm_epsilon)
        result = (gated * factor * norm_gain[None, :]).astype(jnp.bfloat16)
        return (states[-1], result)
    start_state = jnp.zeros((N,), jnp.float32)
    final_state, results = lax.scan(advance, start_state, (input_blocks, gate_blocks, step_blocks))
    return results.reshape(TOKENS, N)
```

```python
import functools

import jax
import jax.numpy as jnp
from jax import lax
from jax.experimental import pallas as pl
from jax.experimental.pallas import tpu as pltpu
from jax.sharding import PartitionSpec as P

MESH = pl.DeviceIdType.MESH
norm_epsilon = 1e-05
LOG2E = 1.4426950408889634

TOK = 512
SUB = 128
CH = 2048
N = 8192
HL = 16
HEADS = 64
GR = 16
NG = SUB // GR
FIRST = 3
SECOND = 8


def drive_factor(widened):
    t = jnp.tanh(widened)
    two_t = t + t
    return two_t * lax.rsqrt(two_t + two_t * t + 1e-37)


def scan_rows(a, b, row):
    for s in (1, 2, 4):
        keep = row >= s
        b = b + a * jnp.where(keep, pltpu.roll(b, s, 0), 0.0)
        a = a * jnp.where(keep, pltpu.roll(a, s, 0), 1.0)
    return a, b


def kernel(
    x_hbm, gate_hbm, steps_hbm, rates_hbm, skip_hbm, gain_hbm, out_hbm,
    x_local, x_all, gate, steps, steps_all, rates, skip, gain,
    spread, later, wide, rest, ends, falls, carry_box, start_box, start_all,
    decay, factor, silu, carry, gated, result,
    local_sem, out_sem, bulk_send, bulk_recv, step_send, step_recv,
    carry_send, carry_recv, start_send, start_recv,
):
    tm, chan = lax.axis_index("tm"), lax.axis_index("chan")
    places = (tm % 4, (tm // 4) % 4, tm // 16)
    strides = (1, 4, 16)

    def chan_peer(r):
        return ((chan // 2 + r // 2) % 2) * 2 + (chan % 2 + r % 2) % 2

    def tm_peer(stage, r):
        here = places[stage]
        return tm + ((here + r) % 4 - here) * strides[stage]

    barrier = pltpu.get_barrier_semaphore()
    for r in (1, 2, 3):
        pl.semaphore_signal(
            barrier, inc=1, device_id={"tm": tm, "chan": chan_peer(r)}, device_id_type=MESH
        )
        for stage in range(3):
            pl.semaphore_signal(
                barrier, inc=1, device_id={"tm": tm_peer(stage, r), "chan": chan}, device_id_type=MESH
            )

    my_cols = pl.ds(pl.multiple_of(chan * CH, CH), CH)
    my_rows = pl.ds(pl.multiple_of(chan * SUB, SUB), SUB)
    load_x = pltpu.make_async_copy(x_hbm, x_local, local_sem.at[0])
    load_steps = pltpu.make_async_copy(steps_hbm, steps, local_sem.at[1])
    load_rates = pltpu.make_async_copy(rates_hbm, rates, local_sem.at[2])
    load_own = pltpu.make_async_copy(x_hbm.at[my_rows], x_all.at[:, my_cols], local_sem.at[3])
    load_gate = pltpu.make_async_copy(gate_hbm, gate, local_sem.at[4])
    load_skip = pltpu.make_async_copy(skip_hbm, skip, local_sem.at[5])
    load_gain = pltpu.make_async_copy(gain_hbm, gain, local_sem.at[6])
    load_own_steps = pltpu.make_async_copy(
        steps_hbm.at[my_rows], steps_all.at[chan], local_sem.at[7]
    )
    for load in (load_x, load_steps, load_rates, load_own, load_own_steps, load_gate, load_skip, load_gain):
        load.start()

    spread[...] = jnp.where(
        lax.broadcasted_iota(jnp.int32, (HL, CH), 1) // 128
        == lax.broadcasted_iota(jnp.int32, (HL, CH), 0),
        1.0,
        0.0,
    ).astype(jnp.bfloat16)
    later[...] = jnp.where(
        lax.broadcasted_iota(jnp.int32, (SUB, SUB), 1)
        > lax.broadcasted_iota(jnp.int32, (SUB, SUB), 0),
        1.0,
        0.0,
    ).astype(jnp.bfloat16)

    load_x.wait()
    load_steps.wait()
    pl.semaphore_wait(barrier, 12)

    def bulk(r, g):
        peer = chan_peer(r)
        return pltpu.make_async_remote_copy(
            src_ref=x_local.at[pl.ds(pl.multiple_of(peer * SUB + g * GR, GR), GR)],
            dst_ref=x_all.at[pl.ds(g * GR, GR), my_cols],
            send_sem=bulk_send.at[r - 1, g],
            recv_sem=bulk_recv.at[r - 1, g],
            device_id={"tm": tm, "chan": peer},
            device_id_type=MESH,
        )

    def step_copy(r):
        peer = chan_peer(r)
        return pltpu.make_async_remote_copy(
            src_ref=steps.at[pl.ds(pl.multiple_of(peer * SUB, SUB), SUB)],
            dst_ref=steps_all.at[chan],
            send_sem=step_send.at[r - 1],
            recv_sem=step_recv.at[r - 1],
            device_id={"tm": tm, "chan": peer},
            device_id_type=MESH,
        )

    far = [(r, g) for g in range(NG) for r in (2, 3)]
    for r in (1, 2, 3):
        step_copy(r).start()
    for r, g in far[:FIRST]:
        bulk(r, g).start()
    for g in range(NG):
        bulk(1, g).start()

    load_rates.wait()

    def summary(j, _):
        base = pl.multiple_of(j * SUB, SUB)
        here = steps[pl.ds(base, SUB), :]
        for c in range(0, CH, 512):
            w = jnp.dot(here, spread[:, c : c + 512], preferred_element_type=jnp.float32)
            wide[:, c : c + 512] = w
            rest[:, c : c + 512] = jnp.dot(
                later[...], w.astype(jnp.bfloat16), preferred_element_type=jnp.float32
            )

        def head(h, _):
            cols = pl.ds(pl.multiple_of(h * 128, 128), 128)
            rate = rates[pl.ds(chan * HL + h, 1), :]
            w, after = wide[:, cols], rest[:, cols]
            x = x_local[pl.ds(base, SUB), cols].astype(jnp.float32)
            term = jnp.exp2(after * (rate * -LOG2E)) * drive_factor(w * rate) * x
            ends[j, pl.ds(h, 1), :] = jnp.sum(term, axis=0, keepdims=True)
            falls[j, pl.ds(h, 1), :] = jnp.exp2((w[0:1] + after[0:1]) * (rate * -LOG2E))
            return 0

        return lax.fori_loop(0, HL, head, 0)

    lax.fori_loop(0, 4, summary, 0)

    e, d = ends[0], falls[0]
    for j in range(1, 4):
        e, d = ends[j] + falls[j] * e, falls[j] * d

    def carry_copy(stage, r):
        here = places[stage]
        return pltpu.make_async_remote_copy(
            src_ref=carry_box.at[stage, here],
            dst_ref=carry_box.at[stage, here],
            send_sem=carry_send.at[stage, r - 1],
            recv_sem=carry_recv.at[stage, r - 1],
            device_id={"tm": tm_peer(stage, r), "chan": chan},
            device_id_type=MESH,
        )

    def carry_arrival(stage, r):
        there = (places[stage] - r + 4) % 4
        return pltpu.make_async_remote_copy(
            src_ref=carry_box.at[stage, there],
            dst_ref=carry_box.at[stage, there],
            send_sem=carry_send.at[stage, r - 1],
            recv_sem=carry_recv.at[stage, r - 1],
            device_id={"tm": tm_peer(stage, r), "chan": chan},
            device_id_type=MESH,
        )

    before = []
    for stage in range(3):
        here = places[stage]
        carry_box[stage, here, 0] = e
        carry_box[stage, here, 1] = d
        for r in (1, 2, 3):
            carry_copy(stage, r).start()
        if stage == 0:
            for r, g in far[FIRST:SECOND]:
                bulk(r, g).start()
        for r in (1, 2, 3):
            carry_arrival(stage, r).wait_recv()
        pre_e, pre_d = jnp.zeros((HL, 128), jnp.float32), jnp.ones((HL, 128), jnp.float32)
        e, d = pre_e, pre_d
        for p in range(4):
            e_p, d_p = carry_box[stage, p, 0], carry_box[stage, p, 1]
            passed = jnp.full((HL, 128), p, jnp.int32) < here
            pre_e = jnp.where(passed, d_p * pre_e + e_p, pre_e)
            pre_d = jnp.where(passed, d_p * pre_d, pre_d)
            e, d = d_p * e + e_p, d_p * d
        before.append((pre_e, pre_d))
    incoming = before[2][0]
    incoming = before[1][1] * incoming + before[1][0]
    incoming = before[0][1] * incoming + before[0][0]

    now = incoming
    for j in range(4):
        start_box[j] = now
        now = falls[j] * now + ends[j]

    def start_copy(r):
        peer = chan_peer(r)
        return pltpu.make_async_remote_copy(
            src_ref=start_box.at[peer],
            dst_ref=start_all.at[chan],
            send_sem=start_send.at[r - 1],
            recv_sem=start_recv.at[r - 1],
            device_id={"tm": tm, "chan": peer},
            device_id_type=MESH,
        )

    start_all[chan] = start_box[chan]
    for r in (1, 2, 3):
        start_copy(r).start()
    for r, g in far[SECOND:]:
        bulk(r, g).start()

    load_own_steps.wait()
    load_gate.wait()
    load_skip.wait()
    load_gain.wait()
    for r in (1, 2, 3):
        step_copy(r).wait_recv()

    def prepare(i, _):
        k, c = i // 4, (i % 4) * 512
        w = jnp.dot(
            steps_all[k],
            spread[:, pl.ds(pl.multiple_of(c, 512), 512)],
            preferred_element_type=jnp.float32,
        )
        for q in range(4):
            cols = pl.ds(pl.multiple_of(i * 512 + q * 128, 128), 128)
            rate = rates[pl.ds(i * 4 + q, 1), :]
            widened = w[:, q * 128 : q * 128 + 128] * rate
            decay[:, cols] = jnp.exp2(widened * -LOG2E)
            factor[:, cols] = drive_factor(widened)
            half = gate[:, cols].astype(jnp.float32) * 0.5
            silu[:, cols] = half + half * jnp.tanh(half)
        return 0

    lax.fori_loop(0, 16, prepare, 0)

    for r in (1, 2, 3):
        start_copy(r).wait_recv()
    load_own.wait()
    for k in range(4):
        carry[k * HL : (k + 1) * HL, :] = start_all[k]

    row = lax.broadcasted_iota(jnp.int32, (8, 128), 0)

    for g in range(NG):
        for r in (1, 2, 3):
            bulk(r, g).wait_recv()
        rows = slice(g * GR, (g + 1) * GR)

        def head(h, total, rows=rows):
            cols = pl.ds(pl.multiple_of(h * 128, 128), 128)
            x = x_all[rows, cols].astype(jnp.float32)
            a = decay[rows, cols]
            b = factor[rows, cols] * x
            state = carry[pl.ds(h, 1), :]
            parts = []
            for p in range(0, GR, 8):
                a_p, b_p = scan_rows(a[p : p + 8], b[p : p + 8], row)
                s_p = b_p + a_p * state
                state = s_p[7:8]
                parts.append(s_p)
            carry[pl.ds(h, 1), :] = state
            s = jnp.concatenate(parts, axis=0)
            mixed = (s + skip[pl.ds(h, 1), :] * x).astype(jnp.bfloat16).astype(jnp.float32)
            v = mixed * silu[rows, cols]
            gated[:, cols] = v
            return total + v * v

        total = lax.fori_loop(0, HEADS, head, jnp.zeros((GR, 128), jnp.float32), unroll=4)
        mean = jnp.sum(total, axis=1, keepdims=True) * (1.0 / N)
        scale = jnp.broadcast_to(lax.rsqrt(mean + norm_epsilon), (GR, 128))

        def finish(h, _, rows=rows, scale=scale):
            cols = pl.ds(pl.multiple_of(h * 128, 128), 128)
            value = gated[:, cols] * scale * gain[pl.ds(h, 1), :]
            result[rows, cols] = value.astype(jnp.bfloat16)
            return 0

        lax.fori_loop(0, HEADS, finish, 0, unroll=8)
        pltpu.make_async_copy(result.at[rows], out_hbm.at[rows], out_sem.at[g]).start()

    for r in (1, 2, 3):
        step_copy(r).wait_send()
        start_copy(r).wait_send()
        for stage in range(3):
            carry_copy(stage, r).wait_send()
        for g in range(NG):
            bulk(r, g).wait_send()
    for g in range(NG):
        rows = slice(g * GR, (g + 1) * GR)
        pltpu.make_async_copy(result.at[rows], out_hbm.at[rows], out_sem.at[g]).wait()


def per_device(inputs, gate_logits, step_sizes, decay_rates, skip_gain, norm_gain):
    f32, bf16, dma = jnp.float32, jnp.bfloat16, pltpu.SemaphoreType.DMA
    any_spec = pl.BlockSpec(memory_space=pl.ANY)
    return pl.pallas_call(
        kernel,
        out_shape=jax.ShapeDtypeStruct((SUB, N), bf16),
        in_specs=[any_spec] * 6,
        out_specs=any_spec,
        scratch_shapes=[
            pltpu.VMEM((TOK, CH), bf16),
            pltpu.VMEM((SUB, N), bf16),
            pltpu.VMEM((SUB, N), bf16),
            pltpu.VMEM((TOK, HL), bf16),
            pltpu.VMEM((4, SUB, HL), bf16),
            pltpu.VMEM((HEADS, 128), f32),
            pltpu.VMEM((HEADS, 128), f32),
            pltpu.VMEM((HEADS, 128), f32),
            pltpu.VMEM((HL, CH), bf16),
            pltpu.VMEM((SUB, SUB), bf16),
            pltpu.VMEM((SUB, CH), f32),
            pltpu.VMEM((SUB, CH), f32),
            pltpu.VMEM((4, HL, 128), f32),
            pltpu.VMEM((4, HL, 128), f32),
            pltpu.VMEM((3, 4, 2, HL, 128), f32),
            pltpu.VMEM((4, HL, 128), f32),
            pltpu.VMEM((4, HL, 128), f32),
            pltpu.VMEM((SUB, N), f32),
            pltpu.VMEM((SUB, N), f32),
            pltpu.VMEM((SUB, N), f32),
            pltpu.VMEM((HEADS, 128), f32),
            pltpu.VMEM((GR, N), f32),
            pltpu.VMEM((SUB, N), bf16),
            dma((8,)),
            dma((NG,)),
            dma((3, NG)),
            dma((3, NG)),
            dma((3,)),
            dma((3,)),
            dma((3, 3)),
            dma((3, 3)),
            dma((3,)),
            dma((3,)),
        ],
        compiler_params=pltpu.CompilerParams(
            collective_id=0, has_side_effects=True, vmem_limit_bytes=56 * 1024 * 1024
        ),
        name="recurrence",
    )(
        inputs,
        gate_logits,
        step_sizes,
        decay_rates.reshape(HEADS, 128),
        skip_gain.reshape(HEADS, 128),
        norm_gain.reshape(HEADS, 128),
    )


def solution(mesh):
    in_specs = (P("tm", "chan"), P(("tm", "chan"), None), P("tm", "chan"), P(), P(), P())
    out_specs = P(("tm", "chan"), None)
    return jax.shard_map(
        per_device, mesh=mesh, in_specs=in_specs, out_specs=out_specs, check_vma=False
    )
```

```python
import functools

import jax
import jax.numpy as jnp
from jax import lax
from jax.experimental import pallas as pl
from jax.experimental.pallas import tpu as pltpu
from jax.sharding import PartitionSpec as P

MESH = pl.DeviceIdType.MESH
norm_epsilon = 1e-05
LOG2E = 1.4426950408889634

TOK = 512
SUB = 128
CH = 2048
N = 8192
HL = 16
HEADS = 64
GR = 16
NG = SUB // GR
FIRST = 2
PREP = 7


def drive_factor(widened):
    t = jnp.tanh(widened)
    two_t = t + t
    return two_t * lax.rsqrt(two_t + two_t * t + 1e-37)


def widen(head_steps, table):
    return lax.dot_general(
        head_steps, table, (((0,), (0,)), ((), ())), preferred_element_type=jnp.float32
    )


def scan_rows(a, b, row):
    for s in (1, 2, 4):
        keep = row >= s
        b = b + a * jnp.where(keep, pltpu.roll(b, s, 0), 0.0)
        a = a * jnp.where(keep, pltpu.roll(a, s, 0), 1.0)
    return a, b


def kernel(
    x_hbm, gate_hbm, steps_hbm, rates_hbm, skip_hbm, gain_hbm, result,
    x_local, x_all, gate, steps, steps_all, rates, skip, gain,
    spread, by_token, wide, rest, ends, falls, carry_box, start_box, start_all,
    decay, factor, silu, carry, gated,
    local_sem, bulk_send, bulk_recv, step_send, step_recv,
    carry_send, carry_recv, relay_send, relay_recv, start_send, start_recv,
):
    tm, chan = lax.axis_index("tm"), lax.axis_index("chan")
    places = (tm % 4, (tm // 4) % 4, tm // 16)
    strides = (1, 4, 16)

    def chan_peer(r):
        return ((chan // 2 + r // 2) % 2) * 2 + (chan % 2 + r % 2) % 2

    def tm_peer(stage, r):
        here = places[stage]
        return tm + ((here + r) % 4 - here) * strides[stage]

    barrier = pltpu.get_barrier_semaphore()
    for r in (1, 2, 3):
        pl.semaphore_signal(
            barrier, inc=1, device_id={"tm": tm, "chan": chan_peer(r)}, device_id_type=MESH
        )
        for stage in range(3):
            pl.semaphore_signal(
                barrier, inc=1, device_id={"tm": tm_peer(stage, r), "chan": chan}, device_id_type=MESH
            )

    my_cols = pl.ds(pl.multiple_of(chan * CH, CH), CH)
    my_rows = pl.ds(pl.multiple_of(chan * SUB, SUB), SUB)
    load_x = pltpu.make_async_copy(x_hbm, x_local, local_sem.at[0])
    load_steps = pltpu.make_async_copy(steps_hbm, steps, local_sem.at[1])
    load_rates = pltpu.make_async_copy(rates_hbm, rates, local_sem.at[2])
    load_own = pltpu.make_async_copy(x_hbm.at[my_rows], x_all.at[:, my_cols], local_sem.at[3])
    load_gate = pltpu.make_async_copy(gate_hbm, gate, local_sem.at[4])
    load_skip = pltpu.make_async_copy(skip_hbm, skip, local_sem.at[5])
    load_gain = pltpu.make_async_copy(gain_hbm, gain, local_sem.at[6])
    load_own_steps = pltpu.make_async_copy(
        steps_hbm.at[:, my_rows], steps_all.at[chan], local_sem.at[7]
    )
    for load in (load_x, load_steps, load_rates, load_own, load_own_steps, load_gate, load_skip, load_gain):
        load.start()

    for p in range(3):
        spread[p * HL : (p + 1) * HL, :] = jnp.where(
            lax.broadcasted_iota(jnp.int32, (HL, CH), 1) // 128
            == lax.broadcasted_iota(jnp.int32, (HL, CH), 0),
            1.0,
            0.0,
        ).astype(jnp.bfloat16)
    later = jnp.where(
        lax.broadcasted_iota(jnp.int32, (SUB, SUB), 0)
        > lax.broadcasted_iota(jnp.int32, (SUB, SUB), 1),
        1.0,
        0.0,
    ).astype(jnp.bfloat16)

    load_steps.wait()
    for j in range(4):
        here = slice(j * SUB, (j + 1) * SUB)
        own = steps[:, here]
        after = jnp.dot(own, later, preferred_element_type=jnp.float32)
        pieces = []
        for _ in range(3):
            pieces.append(after.astype(jnp.bfloat16).astype(jnp.float32))
            after = after - pieces[-1]
        turned = jnp.concatenate([own.astype(jnp.float32), *pieces], axis=0).T
        by_token[here, :] = turned.astype(jnp.bfloat16)

    load_x.wait()
    pl.semaphore_wait(barrier, 12)

    def bulk(r, g):
        peer = chan_peer(r)
        return pltpu.make_async_remote_copy(
            src_ref=x_local.at[pl.ds(pl.multiple_of(peer * SUB + g * GR, GR), GR)],
            dst_ref=x_all.at[pl.ds(g * GR, GR), my_cols],
            send_sem=bulk_send.at[r - 1, g],
            recv_sem=bulk_recv.at[r - 1, g],
            device_id={"tm": tm, "chan": peer},
            device_id_type=MESH,
        )

    def step_copy(r):
        peer = chan_peer(r)
        return pltpu.make_async_remote_copy(
            src_ref=steps.at[:, pl.ds(pl.multiple_of(peer * SUB, SUB), SUB)],
            dst_ref=steps_all.at[chan],
            send_sem=step_send.at[r - 1],
            recv_sem=step_recv.at[r - 1],
            device_id={"tm": tm, "chan": peer},
            device_id_type=MESH,
        )

    far = [(r, g) for g in range(NG) for r in (2, 3)]
    for r in (1, 2, 3):
        step_copy(r).start()
    started, left = [], []

    def send(count):
        for r, g in far[len(started) : len(started) + count]:
            bulk(r, g).start()
            started.append((r, g))

    def pump(count):
        for _ in range(count):
            r, g = started[len(left)]
            bulk(r, g).wait_send()
            left.append((r, g))
            send(1)

    send(FIRST)
    for g in range(NG):
        bulk(1, g).start()

    def widen_block(i, _):
        cols = pl.ds(pl.multiple_of(i * 256, 256), 256)
        wide[:, cols] = jnp.dot(
            by_token[:, :HL], spread[:HL, cols], preferred_element_type=jnp.float32
        )
        rest[:, cols] = jnp.dot(
            by_token[:, HL:], spread[:, cols], preferred_element_type=jnp.float32
        )
        return 0

    lax.fori_loop(0, CH // 256, widen_block, 0)

    load_rates.wait()

    def summary(j, _):
        base = pl.multiple_of(j * SUB, SUB)
        def head(h, _):
            cols = pl.ds(pl.multiple_of(h * 128, 128), 128)
            rate = rates[pl.ds(chan * HL + h, 1), :]
            w, after = wide[pl.ds(base, SUB), cols], rest[pl.ds(base, SUB), cols]
            x = x_local[pl.ds(base, SUB), cols].astype(jnp.float32)
            term = jnp.exp2(after * (rate * -LOG2E)) * drive_factor(w * rate) * x
            ends[j, pl.ds(h, 1), :] = jnp.sum(term, axis=0, keepdims=True)
            falls[j, pl.ds(h, 1), :] = jnp.exp2((w[0:1] + after[0:1]) * (rate * -LOG2E))
            return 0

        return lax.fori_loop(0, HL, head, 0, unroll=4)

    lax.fori_loop(0, 4, summary, 0)

    def prepare(i, _):
        k, c = i // 4, (i % 4) * 512
        w = widen(steps_all[k], spread[:HL, pl.ds(pl.multiple_of(c, 512), 512)])
        for q in range(4):
            cols = pl.ds(pl.multiple_of(i * 512 + q * 128, 128), 128)
            rate = rates[pl.ds(i * 4 + q, 1), :]
            widened = w[:, q * 128 : q * 128 + 128] * rate
            decay[:, cols] = jnp.exp2(widened * -LOG2E)
            factor[:, cols] = drive_factor(widened)
            half = gate[:, cols].astype(jnp.float32) * 0.5
            silu[:, cols] = half + half * jnp.tanh(half)
        return 0


    e, d = ends[0], falls[0]
    for j in range(1, 4):
        e, d = ends[j] + falls[j] * e, falls[j] * d

    z_lo = places[0]

    def relay_copy(slot, to, at):
        return pltpu.make_async_remote_copy(
            src_ref=carry_box.at[0, slot],
            dst_ref=carry_box.at[0, slot],
            send_sem=relay_send.at[at],
            recv_sem=relay_recv.at[slot],
            device_id={"tm": tm - z_lo + to, "chan": chan},
            device_id_type=MESH,
        )

    own_sends = {0: (1, 2, 3), 1: (0,), 2: (3,), 3: (2, 1, 0)}
    relays = {0: (1, (2, 3)), 1: (0, ()), 2: (3, ()), 3: (2, (1, 0))}

    def carry_copy(stage, r, slot):
        return pltpu.make_async_remote_copy(
            src_ref=carry_box.at[stage, slot],
            dst_ref=carry_box.at[stage, slot],
            send_sem=carry_send.at[stage - 1, r - 1],
            recv_sem=carry_recv.at[stage - 1, r - 1],
            device_id={"tm": tm_peer(stage, r), "chan": chan},
            device_id_type=MESH,
        )

    before = []
    for stage in range(3):
        here = places[stage]
        carry_box[stage, here, 0] = e
        carry_box[stage, here, 1] = d
        if stage == 0:
            for place, targets in own_sends.items():

                @pl.when(z_lo == place)
                def _(place=place, targets=targets):
                    for at, to in enumerate(targets):
                        relay_copy(place, to, at).start()

            send(1)
            load_own_steps.wait()
            load_gate.wait()
            for r in (1, 2, 3):
                step_copy(r).wait_recv()
            lax.fori_loop(0, PREP, prepare, 0)
            for place, (slot, targets) in relays.items():

                @pl.when(z_lo == place)
                def _(slot=slot, targets=targets):
                    relay_copy(slot, 0, 0).wait_recv()
                    for at, to in enumerate(targets):
                        relay_copy(slot, to, 3 + at).start()

            pump(2)
            send(1)
            lax.fori_loop(PREP, 16, prepare, 0)
            for place in range(4):

                @pl.when(z_lo == place)
                def _(place=place):
                    for slot in range(4):
                        if slot not in (place, relays[place][0]):
                            relay_copy(slot, 0, 0).wait_recv()

        else:
            for r in (1, 2, 3):
                carry_copy(stage, r, here).start()
            pump(1)
            for r in (1, 2, 3):
                carry_copy(stage, r, (here - r + 4) % 4).wait_recv()
        pre_e, pre_d = jnp.zeros((HL, 128), jnp.float32), jnp.ones((HL, 128), jnp.float32)
        e, d = pre_e, pre_d
        for p in range(4):
            e_p, d_p = carry_box[stage, p, 0], carry_box[stage, p, 1]
            passed = jnp.full((HL, 128), p, jnp.int32) < here
            pre_e = jnp.where(passed, d_p * pre_e + e_p, pre_e)
            pre_d = jnp.where(passed, d_p * pre_d, pre_d)
            e, d = d_p * e + e_p, d_p * d
        before.append((pre_e, pre_d))
    incoming = before[2][0]
    incoming = before[1][1] * incoming + before[1][0]
    incoming = before[0][1] * incoming + before[0][0]

    now = incoming
    for j in range(4):
        start_box[j] = now
        now = falls[j] * now + ends[j]

    def start_copy(r):
        peer = chan_peer(r)
        return pltpu.make_async_remote_copy(
            src_ref=start_box.at[peer],
            dst_ref=start_all.at[chan],
            send_sem=start_send.at[r - 1],
            recv_sem=start_recv.at[r - 1],
            device_id={"tm": tm, "chan": peer},
            device_id_type=MESH,
        )

    start_all[chan] = start_box[chan]
    for r in (1, 2, 3):
        start_copy(r).start()
    send(2 * NG)

    for r in (1, 2, 3):
        start_copy(r).wait_recv()
    load_own.wait()
    load_skip.wait()
    load_gain.wait()
    for k in range(4):
        carry[k * HL : (k + 1) * HL, :] = start_all[k]

    row = lax.broadcasted_iota(jnp.int32, (8, 128), 0)

    for g in range(NG):
        for r in (1, 2, 3):
            bulk(r, g).wait_recv()
        rows = slice(g * GR, (g + 1) * GR)

        def head(h, total, rows=rows):
            cols = pl.ds(pl.multiple_of(h * 128, 128), 128)
            x = x_all[rows, cols].astype(jnp.float32)
            a = decay[rows, cols]
            b = factor[rows, cols] * x
            state = carry[pl.ds(h, 1), :]
            parts = []
            for p in range(0, GR, 8):
                a_p, b_p = scan_rows(a[p : p + 8], b[p : p + 8], row)
                s_p = b_p + a_p * state
                state = s_p[7:8]
                parts.append(s_p)
            carry[pl.ds(h, 1), :] = state
            s = jnp.concatenate(parts, axis=0)
            mixed = (s + skip[pl.ds(h, 1), :] * x).astype(jnp.bfloat16).astype(jnp.float32)
            v = mixed * silu[rows, cols]
            gated[:, cols] = v
            return total + v * v

        total = lax.fori_loop(0, HEADS, head, jnp.zeros((GR, 128), jnp.float32), unroll=4)
        mean = jnp.sum(total, axis=1, keepdims=True) * (1.0 / N)
        scale = jnp.broadcast_to(lax.rsqrt(mean + norm_epsilon), (GR, 128))

        def finish(h, _, rows=rows, scale=scale):
            cols = pl.ds(pl.multiple_of(h * 128, 128), 128)
            value = gated[:, cols] * scale * gain[pl.ds(h, 1), :]
            result[rows, cols] = value.astype(jnp.bfloat16)
            return 0

        lax.fori_loop(0, HEADS, finish, 0, unroll=8)

    for r in (1, 2, 3):
        step_copy(r).wait_send()
        start_copy(r).wait_send()
        for stage in (1, 2):
            carry_copy(stage, r, places[stage]).wait_send()
        for g in range(NG):
            if (r, g) not in left:
                bulk(r, g).wait_send()
    for place in range(4):

        @pl.when(z_lo == place)
        def _(place=place):
            for at in range(len(own_sends[place])):
                relay_copy(place, 0, at).wait_send()
            if len(relays[place][1]):
                for at in range(2):
                    relay_copy(place, 0, 3 + at).wait_send()


def per_device(inputs, gate_logits, step_sizes, decay_rates, skip_gain, norm_gain):
    f32, bf16, dma = jnp.float32, jnp.bfloat16, pltpu.SemaphoreType.DMA
    any_spec = pl.BlockSpec(memory_space=pltpu.HBM)
    return pl.pallas_call(
        kernel,
        out_shape=jax.ShapeDtypeStruct((SUB, N), bf16),
        in_specs=[any_spec] * 6,
        out_specs=pl.BlockSpec(memory_space=pltpu.VMEM),
        scratch_shapes=[
            pltpu.VMEM((TOK, CH), bf16),
            pltpu.VMEM((SUB, N), bf16),
            pltpu.VMEM((SUB, N), bf16),
            pltpu.VMEM((HL, TOK), bf16),
            pltpu.VMEM((4, HL, SUB), bf16),
            pltpu.VMEM((HEADS, 128), f32),
            pltpu.VMEM((HEADS, 128), f32),
            pltpu.VMEM((HEADS, 128), f32),
            pltpu.VMEM((3 * HL, CH), bf16),
            pltpu.VMEM((TOK, 4 * HL), bf16),
            pltpu.VMEM((TOK, CH), f32),
            pltpu.VMEM((TOK, CH), f32),
            pltpu.VMEM((4, HL, 128), f32),
            pltpu.VMEM((4, HL, 128), f32),
            pltpu.VMEM((3, 4, 2, HL, 128), f32),
            pltpu.VMEM((4, HL, 128), f32),
            pltpu.VMEM((4, HL, 128), f32),
            pltpu.VMEM((SUB, N), f32),
            pltpu.VMEM((SUB, N), f32),
            pltpu.VMEM((SUB, N), f32),
            pltpu.VMEM((HEADS, 128), f32),
            pltpu.VMEM((GR, N), f32),
            dma((8,)),
            dma((3, NG)),
            dma((3, NG)),
            dma((3,)),
            dma((3,)),
            dma((2, 3)),
            dma((2, 3)),
            dma((5,)),
            dma((4,)),
            dma((3,)),
            dma((3,)),
        ],
        compiler_params=pltpu.CompilerParams(
            collective_id=0, has_side_effects=True, vmem_limit_bytes=40 * 1024 * 1024
        ),
        name="recurrence",
    )(
        *(
            pltpu.with_memory_space_constraint(operand, pltpu.HBM)
            for operand in (
                inputs,
                gate_logits,
                step_sizes.T,
                decay_rates.reshape(HEADS, 128),
                skip_gain.reshape(HEADS, 128),
                norm_gain.reshape(HEADS, 128),
            )
        )
    )


def solution(mesh):
    in_specs = (P("tm", "chan"), P(("tm", "chan"), None), P("tm", "chan"), P(), P(), P())
    out_specs = P(("tm", "chan"), None)
    return jax.shard_map(
        per_device, mesh=mesh, in_specs=in_specs, out_specs=out_specs, check_vma=False
    )
```
